32 devices in a mesh: task: 2 (over core), row: 16 (over z, y, x).
Axes of the slice: x: 2, y: 2, z: 4, core: 2. Of those that a mesh axis runs over, the one named last changes fastest.
Arguments:
- activation_grams: float32 [2, 7168, 7168], P('task', 'row'), may hold values from -240 to 240, as said below
- adjusted_weights: bfloat16 [2, 7168, 2048], P('task', 'row'), may hold values from -0.59765625 to 0.59765625
Outputs:
- reduced_gram: float32 [7168, 7168], P('row')
- reduced_rhs: float32 [7168, 2048], P('row')
The draws below stay inside these ranges and needn't reach their ends.
Inputs may be any that keep to these rules, and one draw needn't show every extreme that they name: Each activation_grams[m] is symmetric and positive definite.
All inputs are finite; a program needn't handle non-finite values.
Results may differ from the reference program's by a relative error of at most 0.0003.
Values may be sent and summed in bfloat16 or wider, within the bound.
No kernel may reach another device: no remote copies, remote signals or barrier semaphores. Data moves between devices by JAX's collectives and lax.ppermute only.
A program may use at most 192 MiB of HBM per device.

```python
import math
import jax
import jax.numpy as jnp
from jax import lax

H = 7168
DC = 2048
MODELS = 2
PANEL_STEPS = 2
N_ROW = 16


def draw_activation_grams(key, part):
    loading_key, scale_key = jax.random.split(jax.random.fold_in(key, 11))
    strong_rank = 8
    broad_rank = H + 1024
    base_share = 0.25
    strong_share = 0.5
    broad_share = 0.25
    spread_log = math.log(10.0)
    column_scale = jnp.concatenate([jnp.full((strong_rank,), math.sqrt(strong_share / strong_rank), jnp.float32), jnp.full((broad_rank,), math.sqrt(broad_share / broad_rank), jnp.float32)])

    def one_model(model_key):
        loadings = jax.random.normal(model_key, (H, strong_rank + broad_rank), jnp.float32) * column_scale
        shared = jnp.dot(loadings, loadings.T, precision=lax.Precision.HIGHEST)
        return 0.5 * (shared + shared.T)
    common = lax.map(one_model, jax.random.split(loading_key, MODELS))
    correlated = common + base_share * jnp.eye(H, dtype=jnp.float32)
    position = jnp.arange(H, dtype=jnp.float32) / H
    roughness = jnp.exp(jax.random.uniform(scale_key, (MODELS, H), jnp.float32, 0.0, spread_log))
    rooted = jnp.sqrt(roughness * jnp.exp(math.log(3.0) * position))
    return (rooted[:, :, None] * correlated * rooted[:, None, :]).astype(jnp.float32)


def block_levels(key, shape, pieces, low, largest):
    def one(dim, shards_of):
        steps = jax.random.uniform(jax.random.fold_in(jax.random.fold_in(key, 6), dim), (shards_of,), jnp.float32, low / len(pieces), largest / len(pieces))
        return jnp.repeat(jnp.exp(steps), shape[dim] // shards_of).reshape((-1,) + (1,) * (len(shape) - dim - 1))

    loudness = one(*pieces[0])
    for cut in pieces[1:]:
        loudness = loudness * one(*cut)
    return loudness


def gaussian(stream_key, extent, scale, most, pieces=(), held_as=jnp.bfloat16):
    values = scale * jax.random.normal(stream_key, extent, jnp.float32)
    if pieces:
        values = values * block_levels(stream_key, extent, pieces, -0.22, 0.18)
    return jnp.clip(values, -most, most).astype(held_as)


def setup_inputs(seed: int = 0) -> dict:
    arg_keys = jax.random.split(jax.random.key(seed), 3)
    activation_grams = draw_activation_grams(jax.random.fold_in(arg_keys[2], 71), 0)
    adjusted_weights = gaussian(arg_keys[1], (MODELS, H, DC), 0.1, 0.59765625, ((0, 2), (1, 16)))
    return {"activation_grams": activation_grams, "adjusted_weights": adjusted_weights}


def reference(activation_grams, adjusted_weights):
    rows = H // N_ROW
    merged = jnp.zeros((H, H), jnp.float32)
    rhs = jnp.zeros((H, DC), jnp.float32)
    for model in range(MODELS):
        gram = activation_grams[model]
        diagonal_entries = jnp.diagonal(gram)
        scaling = H / jnp.sum(diagonal_entries)
        regular = scaling * (0.9 * gram + 0.1 * jnp.diag(diagonal_entries))
        merged = merged + regular
        rhs = rhs + jnp.dot(regular, adjusted_weights[model].astype(jnp.float32), precision=lax.Precision.HIGHEST)
    for panel in range(PANEL_STEPS):
        low = panel * rows
        high = low + rows
        factor = jnp.linalg.cholesky(merged[low:high, low:high])
        upper = jax.scipy.linalg.solve_triangular(factor, merged[low:high], lower=True)
        solved = jax.scipy.linalg.solve_triangular(factor, rhs[low:high], lower=True)
        below = upper[:, high:].T
        merged = jnp.concatenate([merged[:low], upper, merged[high:] - jnp.dot(below, upper, precision=lax.Precision.HIGHEST)], axis=0)
        rhs = jnp.concatenate([rhs[:low], solved, rhs[high:] - jnp.dot(below, solved, precision=lax.Precision.HIGHEST)], axis=0)
    return (merged, rhs)
```

```python
import functools
import itertools
import math

import jax
import jax.numpy as jnp
from jax import lax
from jax.experimental import pallas as pl
from jax.experimental.pallas import tpu as pltpu
from jax.sharding import PartitionSpec as P


PANEL_STEPS = 2
BLOCK = 128
GROUP = 8
EXACT = lax.Precision.HIGHEST
THREE = lax.Precision.HIGH


def dot(a, b, dims, precision):
    return lax.dot_general(
        a, b, (dims, ((), ())), precision=precision, preferred_element_type=jnp.float32
    )


def invert_block(d_ref, x_ref):
    row = lax.broadcasted_iota(jnp.int32, (BLOCK, BLOCK), 0)
    lane = lax.broadcasted_iota(jnp.int32, (BLOCK, BLOCK), 1)
    x_ref[...] = jnp.where(row == lane, 1.0, 0.0).astype(jnp.float32)
    lanes = lax.broadcasted_iota(jnp.int32, (GROUP, BLOCK), 1)

    def body(step, carry):
        top = d_ref[0:GROUP, :]
        mirror = x_ref[0:GROUP, :]
        small = {}
        for i in range(GROUP):
            for k in range(i, GROUP):
                small[i, k] = jnp.broadcast_to(top[i : i + 1, k : k + 1], (1, BLOCK))
        us = [top[i : i + 1, :] for i in range(GROUP)]
        xs = [mirror[i : i + 1, :] for i in range(GROUP)]
        for i in range(GROUP):
            pivot = small[i, i]
            root = lax.rsqrt(pivot)
            root = root * (1.5 - 0.5 * pivot * root * root)
            us[i] = us[i] * root
            xs[i] = xs[i] * root
            ratio = {k: small[i, k] * root for k in range(i + 1, GROUP)}
            for k in range(i + 1, GROUP):
                for j in range(k, GROUP):
                    small[k, j] = small[k, j] - ratio[k] * ratio[j]
                us[k] = us[k] - ratio[k] * us[i]
                xs[k] = xs[k] - ratio[k] * xs[i]
        u = jnp.concatenate(us, axis=0)
        x = jnp.concatenate(xs, axis=0)
        left = jnp.where(lanes < BLOCK - GROUP * step, u, 0.0)
        d_new = d_ref[GROUP:, :] - dot(left, u, ((0,), (0,)), EXACT)[GROUP:, :]
        x_new = x_ref[GROUP:, :] - dot(left, x, ((0,), (0,)), EXACT)[GROUP:, :]
        d_ref[0 : BLOCK - GROUP, :] = pltpu.roll(d_new, BLOCK - GROUP, 1)
        d_ref[BLOCK - GROUP :, :] = jnp.zeros((GROUP, BLOCK), jnp.float32)
        x_ref[0 : BLOCK - GROUP, :] = x_new
        x_ref[BLOCK - GROUP :, :] = x
        return carry

    lax.fori_loop(0, BLOCK // GROUP, body, 0)


def factor_body(blocks, a_ref, done_ref, w_ref, out_ref, d_ref, x_ref):
    n = a_ref.shape[0]
    w_ref[...] = a_ref[...]
    out_ref[...] = done_ref[...]
    for low in blocks:
        high = low + BLOCK
        d_ref[...] = w_ref[low:high, low:high]
        invert_block(d_ref, x_ref)
        x = x_ref[...]
        out_ref[low:high, low:high] = x
        if low:
            out_ref[low:high, :low] = dot(x, out_ref[low:high, :low], ((1,), (0,)), EXACT)
        if high < n:
            below = dot(w_ref[high:, low:high], x, ((1,), (1,)), EXACT)
            w_ref[high:, high:] = w_ref[high:, high:] - dot(below, below, ((1,), (1,)), EXACT)
            out_ref[high:, :high] = out_ref[high:, :high] - dot(
                below, out_ref[low:high, :high], ((1,), (0,)), EXACT
            )


def eliminate(blocks, a, done):
    n = a.shape[0]
    whole = jax.ShapeDtypeStruct((n, n), jnp.float32)
    return pl.pallas_call(
        functools.partial(factor_body, blocks),
        out_shape=(whole, whole),
        scratch_shapes=[
            pltpu.VMEM((BLOCK, BLOCK), jnp.float32),
            pltpu.VMEM((BLOCK, BLOCK), jnp.float32),
        ],
        cost_estimate=pl.CostEstimate(
            flops=20_000_000_000, bytes_accessed=16 * n * n, transcendentals=n
        ),
    )(a, done)


def inverse_factor(a):
    n = a.shape[0]
    full = -(-n // BLOCK) * BLOCK
    if full != n:
        index = jnp.arange(full)
        a = jnp.pad(a, ((0, full - n), (0, full - n)))
        a = jnp.where((index[:, None] == index[None, :]) & (index[:, None] >= n), 1.0, a)
    blocks = range(0, full, BLOCK)
    cut = len(blocks) // 2
    rest, done = eliminate(blocks[:cut], a, jnp.zeros((full, full), jnp.float32))
    done = eliminate(blocks[cut:], rest, done)[1]
    return done[:n, :n]


def torus_of(count):
    side = math.isqrt(count // 4) if count % 4 == 0 else 0
    return (4, side, side) if side and 4 * side * side == count else (count, 1, 1)


def shifted(value, torus, dim, by):
    pairs = []
    count = math.prod(torus)
    inner = math.prod(torus[dim + 1 :])
    size = torus[dim]
    for source in range(count):
        at = (source // inner) % size
        pairs.append((source, source + ((at + by) % size - at) * inner))
    return lax.ppermute(value, "row", pairs)


def blank(shape, dtype):
    return pl.pallas_call(
        lambda out_ref: None,
        out_shape=jax.ShapeDtypeStruct(shape, dtype),
        out_specs=pl.BlockSpec(memory_space=pl.ANY),
    )()


def along(torus, dim):
    return (lax.axis_index("row") // math.prod(torus[dim + 1 :])) % torus[dim]


def arrivals(value, torus, dim):
    size = torus[dim]
    at = along(torus, dim)
    items = []
    up = down = value
    for step in range(1, (size - 1) // 2 + 1):
        up = shifted(up, torus, dim, 1)
        down = shifted(down, torus, dim, -1)
        items += [(up, {dim: (at - step) % size}), (down, {dim: (at + step) % size})]
    if size == 2:
        items.append((shifted(value, torus, dim, 1), {dim: 1 - at}))
    elif size % 2 == 0:
        cut = next((d for d in range(3) if value.shape[d] % 2 == 0), 3)
        half = value.shape[cut] // 2
        far = (at + size // 2) % size
        first = shifted(lax.slice_in_dim(up, 0, half, axis=cut), torus, dim, 1)
        second = lax.slice_in_dim(down, half, value.shape[cut], axis=cut)
        second = shifted(second, torus, dim, -1)
        items += [(first, {dim: far}), (second, {dim: far, cut: half})]
    return items


def fill(buffer, items, lane=0):
    for chunk, at in items:
        start = [at.get(d, 0) for d in range(4)] + [lane]
        buffer = lax.dynamic_update_slice(
            buffer, chunk, tuple(jnp.asarray(i, jnp.int32) for i in start)
        )
    return buffer


def moved(items, by):
    return [(chunk, {**at, 0: at.get(0, 0) + by}) for chunk, at in items]


def gather_along(value, torus, dim):
    shape = list(value.shape)
    shape[dim] = torus[dim]
    buffer = fill(blank(tuple(shape), value.dtype), [(value, {dim: along(torus, dim)})])
    return fill(buffer, arrivals(value, torus, dim))


def widths_of(total):
    unit = 128 if total % 128 == 0 and total >= 512 else 1
    last = total // unit // 4 if total // unit >= 12 else total // unit // 7
    first = (total // unit - last) // 2
    return (first * unit, total - (first + last) * unit, last * unit)


def after(value, *others):
    return lax.optimization_barrier((value, *others))[0]


def torus_sum(value, torus, dims):
    total = value
    for shift in itertools.product(*(range(torus[d]) for d in dims)):
        if any(shift):
            pairs = []
            for source in range(math.prod(torus)):
                target = source
                for d, by in zip(dims, shift):
                    inner = math.prod(torus[d + 1 :])
                    at = (source // inner) % torus[d]
                    target += ((at + by) % torus[d] - at) * inner
                pairs.append((source, target))
            total = total + lax.ppermute(value, "row", pairs)
    return total


def spread(shard):
    return shard.reshape((1, 1, 1) + shard.shape)


def swapped(value):
    return lax.ppermute(value, "task", [(0, 1), (1, 0)])


def per_device(activation_grams, adjusted_weights):
    gram, weights = activation_grams[0], adjusted_weights[0]
    rows, width = gram.shape
    columns = weights.shape[1]
    panel = PANEL_STEPS * rows
    torus = torus_of(width // rows)
    position = lax.axis_index("row")
    start = position * rows

    def is_diagonal(shape, first):
        row = lax.broadcasted_iota(jnp.int32, shape, 0) + first
        return row == lax.broadcasted_iota(jnp.int32, shape, 1)

    def damped(block):
        return jnp.where(is_diagonal(block.shape, position * rows), block, 0.9 * block)

    reach = min(width, -(-rows // 128) * 128 + 128)
    first = jnp.minimum(start // 128 * 128, width - reach)
    near = lax.dynamic_slice_in_dim(gram, first, reach, 1)
    own_trace = jnp.sum(jnp.where(is_diagonal(near.shape, start - first), near, 0.0))
    trace = torus_sum(jnp.full((8, 128), own_trace), torus, (0,))

    own_panel = damped(gram[:, :panel])
    size0, size1, _ = widths_of(panel)
    split = size0 + size1
    late = gather_along(spread(own_panel[:, split:]), torus, 2)
    late = gather_along(late, torus, 1)
    early = gather_along(spread(own_panel[:, :split]), torus, 0)
    trace = torus_sum(trace, torus, (1, 2))
    scaling = width / trace[:1, :1]
    mid0 = gather_along(early[..., :size0], torus, 2)
    mid1 = gather_along(early[..., size0:], torus, 1)
    last = gather_along(late, torus, 0)
    ahead = arrivals(mid0[:1], torus, 1), arrivals(mid1[:1], torus, 2)
    behind = arrivals(mid0[1:], torus, 1), arrivals(mid1[1:], torus, 2)
    plane = blank((1,) + torus[1:] + (rows, panel), jnp.float32)
    panels = blank(torus + (rows, panel), jnp.float32)
    for lane, value, dim in ((0, mid0, 1), (size0, mid1, 2), (split, last, None)):
        at = {} if dim is None else {dim: along(torus, dim)}
        plane = fill(plane, [(value[:1], at)], lane)
        panels = fill(panels, [(value, at)], lane)
    plane = fill(plane, ahead[0], 0)
    plane = fill(plane, ahead[1], size0)
    panels = fill(panels, ahead[0], 0)
    panels = fill(panels, ahead[1], size0)
    panels = fill(panels, moved(behind[0], 1), 0)
    panels = fill(panels, moved(behind[1], 1), size0)
    panels = panels.reshape(width, panel)

    width0, width1, _ = widths_of(columns)
    fork = width0 + width1
    w_late = gather_along(spread(weights[:, fork:]), torus, 2)
    weights = after(weights, early[:1, :1, :1, :8, :128])
    w_early = gather_along(spread(weights[:, :fork]), torus, 0)
    w_late = gather_along(w_late, torus, 1)
    half0, half1 = width0 // 2, width1 // 2
    w_mids = []
    for turn, (size, dim) in enumerate(((half0, 2), (half1, 1), (width0 - half0, 2), (width1 - half1, 1))):
        first = (0, width0, half0, width0 + half1)[turn]
        w_mids.append(gather_along(w_early[..., first : first + size], torus, dim))
    gathered_weights = [gather_along(w_late, torus, 0)] + [
        gather_along(mid, torus, 1 if turn % 2 == 0 else 2)
        for turn, mid in enumerate(w_mids)
    ]
    gathered_weights = [w.reshape(width, -1) for w in gathered_weights]

    corner = scaling * plane.reshape(-1, panel)[:panel]
    corner = corner + swapped(corner)
    own = scaling * own_panel
    own = own + swapped(own)
    inverse = inverse_factor(corner)
    factored = position < PANEL_STEPS
    lead = lax.dynamic_slice_in_dim(inverse, jnp.minimum(position, PANEL_STEPS - 1) * rows, rows, 0)
    folded = dot(dot(own, inverse, ((1,), (1,)), EXACT), inverse, ((1,), (0,)), EXACT)
    transform = scaling * jnp.where(factored, lead, -folded)
    kept = jnp.where(factored, 0.0, scaling)
    reduced = kept * damped(gram) + dot(transform, panels, ((1,), (1,)), THREE)
    partner = swapped(reduced)
    reduced_gram = reduced + partner

    high = lax.reduce_precision(reduced, 8, 7)
    rest = (reduced - high).astype(jnp.bfloat16)
    both = jnp.concatenate([high.astype(jnp.bfloat16), rest], axis=0)
    solved = []
    for weight in gathered_weights:
        part = jnp.dot(both, weight, preferred_element_type=jnp.float32)
        part = part[:rows] + part[rows:]
        solved.append(part + swapped(part))
    return (reduced_gram, jnp.concatenate([solved[i] for i in (1, 3, 2, 4, 0)], axis=1))


def solution(mesh):
    placed = (P("task", "row", None), P("task", "row", None))
    return jax.shard_map(
        per_device,
        mesh=mesh,
        in_specs=placed,
        out_specs=(P("row", None), P("row", None)),
        check_vma=False,
    )
```

```python
import functools
import itertools
import math

import jax
import jax.numpy as jnp
from jax import lax
from jax.experimental import pallas as pl
from jax.experimental.pallas import tpu as pltpu
from jax.sharding import PartitionSpec as P


PANEL_STEPS = 2
BLOCK = 128
GROUP = 8
EXACT = lax.Precision.HIGHEST
THREE = lax.Precision.HIGH


def dot(a, b, dims, precision):
    return lax.dot_general(
        a, b, (dims, ((), ())), precision=precision, preferred_element_type=jnp.float32
    )


def parts(value):
    high = value.astype(jnp.bfloat16).astype(jnp.float32)
    rest = value - high
    mid = rest.astype(jnp.bfloat16).astype(jnp.float32)
    return high, mid, rest - mid


def rank_update(left, right):
    high, mid, low = parts(left)
    left = jnp.concatenate([high, high, mid, high, mid, low], axis=0).astype(jnp.bfloat16)
    high, mid, low = parts(right)
    right = jnp.concatenate([high, mid, high, low, mid, high], axis=0).astype(jnp.bfloat16)
    return lax.dot_general(
        left, right, (((0,), (0,)), ((), ())), preferred_element_type=jnp.float32
    )


def invert_block(d_ref, x_ref):
    row = lax.broadcasted_iota(jnp.int32, (BLOCK, BLOCK), 0)
    lane = lax.broadcasted_iota(jnp.int32, (BLOCK, BLOCK), 1)
    x_ref[...] = jnp.where(row == lane, 1.0, 0.0).astype(jnp.float32)
    lanes = lax.broadcasted_iota(jnp.int32, (GROUP, BLOCK), 1)

    def body(step, carry):
        top = d_ref[0:GROUP, :]
        mirror = x_ref[0:GROUP, :]
        small = {}
        for i in range(GROUP):
            for k in range(i, GROUP):
                small[i, k] = jnp.broadcast_to(top[i : i + 1, k : k + 1], (1, BLOCK))
        us = [top[i : i + 1, :] for i in range(GROUP)]
        xs = [mirror[i : i + 1, :] for i in range(GROUP)]
        for i in range(GROUP):
            pivot = small[i, i]
            root = lax.rsqrt(pivot)
            us[i] = us[i] * root
            xs[i] = xs[i] * root
            ratio = {k: small[i, k] * root for k in range(i + 1, GROUP)}
            for k in range(i + 1, GROUP):
                for j in range(k, GROUP):
                    small[k, j] = small[k, j] - ratio[k] * ratio[j]
                us[k] = us[k] - ratio[k] * us[i]
                xs[k] = xs[k] - ratio[k] * xs[i]
        u = jnp.concatenate(us, axis=0)
        x = jnp.concatenate(xs, axis=0)
        left = jnp.where(lanes < BLOCK - GROUP * step, u, 0.0)
        gone = rank_update(left, jnp.concatenate([u, x], axis=1))
        d_new = d_ref[GROUP:, :] - gone[GROUP:, :BLOCK]
        x_new = x_ref[GROUP:, :] - gone[GROUP:, BLOCK:]
        d_ref[0 : BLOCK - GROUP, :] = pltpu.roll(d_new, BLOCK - GROUP, 1)
        d_ref[BLOCK - GROUP :, :] = jnp.zeros((GROUP, BLOCK), jnp.float32)
        x_ref[0 : BLOCK - GROUP, :] = x_new
        x_ref[BLOCK - GROUP :, :] = x
        return carry

    lax.fori_loop(0, BLOCK // GROUP, body, 0)


def factor_body(blocks, a_ref, done_ref, w_ref, out_ref, d_ref, x_ref):
    n = a_ref.shape[0]
    w_ref[...] = a_ref[...]
    out_ref[...] = done_ref[...]
    for low in blocks:
        high = low + BLOCK
        d_ref[...] = w_ref[low:high, low:high]
        invert_block(d_ref, x_ref)
        x = x_ref[...]
        out_ref[low:high, low:high] = x
        if low:
            out_ref[low:high, :low] = dot(x, out_ref[low:high, :low], ((1,), (0,)), EXACT)
        if high < n:
            below = dot(w_ref[high:, low:high], x, ((1,), (1,)), EXACT)
            w_ref[high:, high:] = w_ref[high:, high:] - dot(below, below, ((1,), (1,)), EXACT)
            out_ref[high:, :high] = out_ref[high:, :high] - dot(
                below, out_ref[low:high, :high], ((1,), (0,)), EXACT
            )


def eliminate(blocks, a, done):
    n = a.shape[0]
    whole = jax.ShapeDtypeStruct((n, n), jnp.float32)
    return pl.pallas_call(
        functools.partial(factor_body, blocks),
        out_shape=(whole, whole),
        scratch_shapes=[
            pltpu.VMEM((BLOCK, BLOCK), jnp.float32),
            pltpu.VMEM((BLOCK, BLOCK), jnp.float32),
        ],
        cost_estimate=pl.CostEstimate(
            flops=20_000_000_000, bytes_accessed=16 * n * n, transcendentals=n
        ),
    )(a, done)


def inverse_factor(a):
    n = a.shape[0]
    full = -(-n // BLOCK) * BLOCK
    if full != n:
        index = jnp.arange(full)
        a = jnp.pad(a, ((0, full - n), (0, full - n)))
        a = jnp.where((index[:, None] == index[None, :]) & (index[:, None] >= n), 1.0, a)
    blocks = range(0, full, BLOCK)
    cut = len(blocks) // 2
    rest, done = eliminate(blocks[:cut], a, jnp.zeros((full, full), jnp.float32))
    done = eliminate(blocks[cut:], rest, done)[1]
    return done[:n, :n]


def torus_of(count):
    side = math.isqrt(count // 4) if count % 4 == 0 else 0
    return (4, side, side) if side and 4 * side * side == count else (count, 1, 1)


def shifted(value, torus, dim, by):
    pairs = []
    count = math.prod(torus)
    inner = math.prod(torus[dim + 1 :])
    size = torus[dim]
    for source in range(count):
        at = (source // inner) % size
        pairs.append((source, source + ((at + by) % size - at) * inner))
    return lax.ppermute(value, "row", pairs)


def blank(shape, dtype):
    return pl.pallas_call(
        lambda out_ref: None,
        out_shape=jax.ShapeDtypeStruct(shape, dtype),
        out_specs=pl.BlockSpec(memory_space=pl.ANY),
    )()


def along(torus, dim):
    return (lax.axis_index("row") // math.prod(torus[dim + 1 :])) % torus[dim]


def arrivals(value, torus, dim):
    size = torus[dim]
    at = along(torus, dim)
    items = []
    up = down = value
    for step in range(1, (size - 1) // 2 + 1):
        up = shifted(up, torus, dim, 1)
        down = shifted(down, torus, dim, -1)
        items += [(up, {dim: (at - step) % size}), (down, {dim: (at + step) % size})]
    if size == 2:
        items.append((shifted(value, torus, dim, 1), {dim: 1 - at}))
    elif size % 2 == 0:
        cut = next((d for d in range(3) if value.shape[d] % 2 == 0), 3)
        half = value.shape[cut] // 2
        far = (at + size // 2) % size
        first = shifted(lax.slice_in_dim(up, 0, half, axis=cut), torus, dim, 1)
        second = lax.slice_in_dim(down, half, value.shape[cut], axis=cut)
        second = shifted(second, torus, dim, -1)
        items += [(first, {dim: far}), (second, {dim: far, cut: half})]
    return items


def fill(buffer, items, lane=0):
    for chunk, at in items:
        start = [at.get(d, 0) for d in range(4)] + [lane]
        buffer = lax.dynamic_update_slice(
            buffer, chunk, tuple(jnp.asarray(i, jnp.int32) for i in start)
        )
    return buffer


def moved(items, by):
    return [(chunk, {**at, 0: at.get(0, 0) + by}) for chunk, at in items]


def gather_along(value, torus, dim):
    shape = list(value.shape)
    shape[dim] = torus[dim]
    buffer = fill(blank(tuple(shape), value.dtype), [(value, {dim: along(torus, dim)})])
    return fill(buffer, arrivals(value, torus, dim))


def widths_of(total):
    unit = 128 if total % 128 == 0 and total >= 512 else 1
    last = total // unit // 4 if total // unit >= 12 else total // unit // 7
    first = (total // unit - last) // 2
    return (first * unit, total - (first + last) * unit, last * unit)


def after(value, *others):
    return lax.optimization_barrier((value, *others))[0]


def torus_sum(value, torus, dims):
    total = value
    for shift in itertools.product(*(range(torus[d]) for d in dims)):
        if any(shift):
            pairs = []
            for source in range(math.prod(torus)):
                target = source
                for d, by in zip(dims, shift):
                    inner = math.prod(torus[d + 1 :])
                    at = (source // inner) % torus[d]
                    target += ((at + by) % torus[d] - at) * inner
                pairs.append((source, target))
            total = total + lax.ppermute(value, "row", pairs)
    return total


def spread(shard):
    return shard.reshape((1, 1, 1) + shard.shape)


def swapped(value):
    return lax.ppermute(value, "task", [(0, 1), (1, 0)])


def per_device(activation_grams, adjusted_weights):
    gram, weights = activation_grams[0], adjusted_weights[0]
    rows, width = gram.shape
    columns = weights.shape[1]
    panel = PANEL_STEPS * rows
    torus = torus_of(width // rows)
    position = lax.axis_index("row")
    start = position * rows

    def is_diagonal(shape, first):
        row = lax.broadcasted_iota(jnp.int32, shape, 0) + first
        return row == lax.broadcasted_iota(jnp.int32, shape, 1)

    def damped(block):
        return jnp.where(is_diagonal(block.shape, position * rows), block, 0.9 * block)

    reach = min(width, -(-rows // 128) * 128 + 128)
    first = jnp.minimum(start // 128 * 128, width - reach)
    near = lax.dynamic_slice_in_dim(gram, first, reach, 1)
    own_trace = jnp.sum(jnp.where(is_diagonal(near.shape, start - first), near, 0.0))
    trace = torus_sum(jnp.full((8, 128), own_trace), torus, (0,))

    own_panel = damped(gram[:, :panel])
    size0, size1, _ = widths_of(panel)
    split = size0 + size1
    late = gather_along(spread(own_panel[:, split:]), torus, 2)
    late = gather_along(late, torus, 1)
    early = gather_along(spread(own_panel[:, :split]), torus, 0)
    trace = torus_sum(trace, torus, (1, 2))
    scaling = width / trace[:1, :1]
    mid0 = gather_along(early[..., :size0], torus, 2)
    mid1 = gather_along(early[..., size0:], torus, 1)
    last = gather_along(late, torus, 0)
    ahead = arrivals(mid0[:1], torus, 1), arrivals(mid1[:1], torus, 2)
    behind = arrivals(mid0[1:], torus, 1), arrivals(mid1[1:], torus, 2)
    plane = blank((1,) + torus[1:] + (rows, panel), jnp.float32)
    panels = blank(torus + (rows, panel), jnp.float32)
    for lane, value, dim in ((0, mid0, 1), (size0, mid1, 2), (split, last, None)):
        at = {} if dim is None else {dim: along(torus, dim)}
        plane = fill(plane, [(value[:1], at)], lane)
        panels = fill(panels, [(value, at)], lane)
    plane = fill(plane, ahead[0], 0)
    plane = fill(plane, ahead[1], size0)
    panels = fill(panels, ahead[0], 0)
    panels = fill(panels, ahead[1], size0)
    panels = fill(panels, moved(behind[0], 1), 0)
    panels = fill(panels, moved(behind[1], 1), size0)
    panels = panels.reshape(width, panel)

    width0, width1, _ = widths_of(columns)
    fork = width0 + width1
    w_late = gather_along(spread(weights[:, fork:]), torus, 2)
    weights = after(weights, early[:1, :1, :1, :8, :128])
    w_early = gather_along(spread(weights[:, :fork]), torus, 0)
    w_late = gather_along(w_late, torus, 1)
    half0, half1 = width0 // 2, width1 // 2
    w_mids = []
    for turn, (size, dim) in enumerate(((half0, 2), (half1, 1), (width0 - half0, 2), (width1 - half1, 1))):
        first = (0, width0, half0, width0 + half1)[turn]
        w_mids.append(gather_along(w_early[..., first : first + size], torus, dim))
    gathered_weights = [gather_along(w_late, torus, 0)] + [
        gather_along(mid, torus, 1 if turn % 2 == 0 else 2)
        for turn, mid in enumerate(w_mids)
    ]
    gathered_weights = [w.reshape(width, -1) for w in gathered_weights]

    corner = scaling * plane.reshape(-1, panel)[:panel]
    corner = corner + swapped(corner)
    own = scaling * after(own_panel, early[:1, :1, :1, :8, :128])
    own = own + swapped(own)
    inverse = inverse_factor(corner)
    factored = position < PANEL_STEPS
    lead = lax.dynamic_slice_in_dim(inverse, jnp.minimum(position, PANEL_STEPS - 1) * rows, rows, 0)
    folded = dot(dot(own, inverse, ((1,), (1,)), EXACT), inverse, ((1,), (0,)), EXACT)
    transform = scaling * jnp.where(factored, lead, -folded)
    kept = jnp.where(factored, 0.0, scaling)
    reduced = kept * damped(gram) + dot(transform, panels, ((1,), (1,)), THREE)
    partner = swapped(reduced)
    reduced_gram = reduced + partner

    high = lax.reduce_precision(reduced, 8, 7)
    rest = (reduced - high).astype(jnp.bfloat16)
    both = jnp.concatenate([high.astype(jnp.bfloat16), rest], axis=0)
    solved = []
    for weight in gathered_weights:
        part = jnp.dot(both, weight, preferred_element_type=jnp.float32)
        part = part[:rows] + part[rows:]
        solved.append(part + swapped(part))
    return (reduced_gram, jnp.concatenate([solved[i] for i in (1, 3, 2, 4, 0)], axis=1))


def solution(mesh):
    placed = (P("task", "row", None), P("task", "row", None))
    return jax.shard_map(
        per_device,
        mesh=mesh,
        in_specs=placed,
        out_specs=(P("row", None), P("row", None)),
        check_vma=False,
    )
```

```python
import functools
import itertools
import math

import jax
import jax.numpy as jnp
from jax import lax
from jax.experimental import pallas as pl
from jax.experimental.pallas import tpu as pltpu
from jax.sharding import PartitionSpec as P


PANEL_STEPS = 2
BLOCK = 128
GROUP = 8
EXACT = lax.Precision.HIGHEST
THREE = lax.Precision.HIGH


def dot(a, b, dims, precision):
    return lax.dot_general(
        a, b, (dims, ((), ())), precision=precision, preferred_element_type=jnp.float32
    )


def parts(value):
    high = value.astype(jnp.bfloat16).astype(jnp.float32)
    rest = value - high
    mid = rest.astype(jnp.bfloat16).astype(jnp.float32)
    return high, mid, rest - mid


def rank_update(left, right):
    high, mid, low = parts(left)
    left = jnp.concatenate([high, high, mid, high, mid, low], axis=0).astype(jnp.bfloat16)
    high, mid, low = parts(right)
    right = jnp.concatenate([high, mid, high, low, mid, high], axis=0).astype(jnp.bfloat16)
    return lax.dot_general(
        left, right, (((0,), (0,)), ((), ())), preferred_element_type=jnp.float32
    )


def invert_block(d_ref, x_ref):
    row = lax.broadcasted_iota(jnp.int32, (BLOCK, BLOCK), 0)
    lane = lax.broadcasted_iota(jnp.int32, (BLOCK, BLOCK), 1)
    x_ref[...] = jnp.where(row == lane, 1.0, 0.0).astype(jnp.float32)
    lanes = lax.broadcasted_iota(jnp.int32, (GROUP, BLOCK), 1)

    def body(step, carry):
        top = d_ref[0:GROUP, :]
        mirror = x_ref[0:GROUP, :]
        small = {}
        for i in range(GROUP):
            for k in range(i, GROUP):
                small[i, k] = jnp.broadcast_to(top[i : i + 1, k : k + 1], (1, BLOCK))
        us = [top[i : i + 1, :] for i in range(GROUP)]
        xs = [mirror[i : i + 1, :] for i in range(GROUP)]
        for i in range(GROUP):
            pivot = small[i, i]
            root = lax.rsqrt(pivot)
            us[i] = us[i] * root
            xs[i] = xs[i] * root
            ratio = {k: small[i, k] * root for k in range(i + 1, GROUP)}
            for k in range(i + 1, GROUP):
                for j in range(k, GROUP):
                    small[k, j] = small[k, j] - ratio[k] * ratio[j]
                us[k] = us[k] - ratio[k] * us[i]
                xs[k] = xs[k] - ratio[k] * xs[i]
        u = jnp.concatenate(us, axis=0)
        x = jnp.concatenate(xs, axis=0)
        left = jnp.where(lanes < BLOCK - GROUP * step, u, 0.0)
        gone = rank_update(left, jnp.concatenate([u, x], axis=1))
        d_new = d_ref[GROUP:, :] - gone[GROUP:, :BLOCK]
        x_new = x_ref[GROUP:, :] - gone[GROUP:, BLOCK:]
        d_ref[0 : BLOCK - GROUP, :] = pltpu.roll(d_new, BLOCK - GROUP, 1)
        d_ref[BLOCK - GROUP :, :] = jnp.zeros((GROUP, BLOCK), jnp.float32)
        x_ref[0 : BLOCK - GROUP, :] = x_new
        x_ref[BLOCK - GROUP :, :] = x
        return carry

    lax.fori_loop(0, BLOCK // GROUP, body, 0)


def factor_body(blocks, a_ref, done_ref, w_ref, out_ref, d_ref, x_ref):
    n = a_ref.shape[0]
    w_ref[...] = a_ref[...]
    out_ref[...] = done_ref[...]
    for low in blocks:
        high = low + BLOCK
        d_ref[...] = w_ref[low:high, low:high]
        invert_block(d_ref, x_ref)
        x = x_ref[...]
        out_ref[low:high, low:high] = x
        if low:
            out_ref[low:high, :low] = dot(x, out_ref[low:high, :low], ((1,), (0,)), EXACT)
        if high < n:
            below = dot(w_ref[high:, low:high], x, ((1,), (1,)), EXACT)
            w_ref[high:, high:] = w_ref[high:, high:] - dot(below, below, ((1,), (1,)), EXACT)
            out_ref[high:, :high] = out_ref[high:, :high] - dot(
                below, out_ref[low:high, :high], ((1,), (0,)), EXACT
            )


def eliminate(blocks, a, done):
    n = a.shape[0]
    whole = jax.ShapeDtypeStruct((n, n), jnp.float32)
    return pl.pallas_call(
        functools.partial(factor_body, blocks),
        out_shape=(whole, whole),
        scratch_shapes=[
            pltpu.VMEM((BLOCK, BLOCK), jnp.float32),
            pltpu.VMEM((BLOCK, BLOCK), jnp.float32),
        ],
        cost_estimate=pl.CostEstimate(
            flops=20_000_000_000, bytes_accessed=16 * n * n, transcendentals=n
        ),
    )(a, done)


def inverse_factor(a):
    n = a.shape[0]
    full = -(-n // BLOCK) * BLOCK
    if full != n:
        index = jnp.arange(full)
        a = jnp.pad(a, ((0, full - n), (0, full - n)))
        a = jnp.where((index[:, None] == index[None, :]) & (index[:, None] >= n), 1.0, a)
    blocks = range(0, full, BLOCK)
    cut = len(blocks) // 2
    rest, done = eliminate(blocks[:cut], a, jnp.zeros((full, full), jnp.float32))
    done = eliminate(blocks[cut:], rest, done)[1]
    return done[:n, :n]


def torus_of(count):
    side = math.isqrt(count // 4) if count % 4 == 0 else 0
    return (4, side, side) if side and 4 * side * side == count else (count, 1, 1)


def shifted(value, torus, dim, by):
    pairs = []
    count = math.prod(torus)
    inner = math.prod(torus[dim + 1 :])
    size = torus[dim]
    for source in range(count):
        at = (source // inner) % size
        pairs.append((source, source + ((at + by) % size - at) * inner))
    return lax.ppermute(value, "row", pairs)


def blank(shape, dtype):
    return pl.pallas_call(
        lambda out_ref: None,
        out_shape=jax.ShapeDtypeStruct(shape, dtype),
        out_specs=pl.BlockSpec(memory_space=pl.ANY),
    )()


def along(torus, dim):
    return (lax.axis_index("row") // math.prod(torus[dim + 1 :])) % torus[dim]


def arrivals(value, torus, dim):
    size = torus[dim]
    at = along(torus, dim)
    items = []
    up = down = value
    for step in range(1, (size - 1) // 2 + 1):
        up = shifted(up, torus, dim, 1)
        down = shifted(down, torus, dim, -1)
        items += [(up, {dim: (at - step) % size}), (down, {dim: (at + step) % size})]
    if size == 2:
        items.append((shifted(value, torus, dim, 1), {dim: 1 - at}))
    elif size % 2 == 0:
        cut = next((d for d in range(3) if value.shape[d] % 2 == 0), 3)
        half = value.shape[cut] // 2
        far = (at + size // 2) % size
        first = shifted(lax.slice_in_dim(up, 0, half, axis=cut), torus, dim, 1)
        second = lax.slice_in_dim(down, half, value.shape[cut], axis=cut)
        second = shifted(second, torus, dim, -1)
        items += [(first, {dim: far}), (second, {dim: far, cut: half})]
    return items


def fill(buffer, items, lane=0):
    for chunk, at in items:
        start = [at.get(d, 0) for d in range(4)] + [lane]
        buffer = lax.dynamic_update_slice(
            buffer, chunk, tuple(jnp.asarray(i, jnp.int32) for i in start)
        )
    return buffer


def moved(items, by):
    return [(chunk, {**at, 0: at.get(0, 0) + by}) for chunk, at in items]


def gather_along(value, torus, dim):
    shape = list(value.shape)
    shape[dim] = torus[dim]
    buffer = fill(blank(tuple(shape), value.dtype), [(value, {dim: along(torus, dim)})])
    return fill(buffer, arrivals(value, torus, dim))


def widths_of(total):
    unit = 128 if total % 128 == 0 and total >= 512 else 1
    last = total // unit // 4 if total // unit >= 12 else total // unit // 7
    first = (total // unit - last) // 2
    return (first * unit, total - (first + last) * unit, last * unit)


def after(value, *others):
    return lax.optimization_barrier((value, *others))[0]


def torus_sum(value, torus, dims):
    total = value
    for shift in itertools.product(*(range(torus[d]) for d in dims)):
        if any(shift):
            pairs = []
            for source in range(math.prod(torus)):
                target = source
                for d, by in zip(dims, shift):
                    inner = math.prod(torus[d + 1 :])
                    at = (source // inner) % torus[d]
                    target += ((at + by) % torus[d] - at) * inner
                pairs.append((source, target))
            total = total + lax.ppermute(value, "row", pairs)
    return total


def spread(shard):
    return shard.reshape((1, 1, 1) + shard.shape)


def swapped(value):
    return lax.ppermute(value, "task", [(0, 1), (1, 0)])


def per_device(activation_grams, adjusted_weights):
    gram, weights = activation_grams[0], adjusted_weights[0]
    rows, width = gram.shape
    columns = weights.shape[1]
    panel = PANEL_STEPS * rows
    torus = torus_of(width // rows)
    position = lax.axis_index("row")
    start = position * rows

    def is_diagonal(shape, first):
        row = lax.broadcasted_iota(jnp.int32, shape, 0) + first
        return row == lax.broadcasted_iota(jnp.int32, shape, 1)

    def damped(block):
        return jnp.where(is_diagonal(block.shape, position * rows), block, 0.9 * block)

    reach = min(width, -(-rows // 128) * 128 + 128)
    first = jnp.minimum(start // 128 * 128, width - reach)
    near = lax.dynamic_slice_in_dim(gram, first, reach, 1)
    own_trace = jnp.sum(jnp.where(is_diagonal(near.shape, start - first), near, 0.0))
    trace = torus_sum(jnp.full((8, 128), own_trace), torus, (0,))

    own_panel = damped(gram[:, :panel])
    size0, size1, _ = widths_of(panel)
    split = size0 + size1
    late = gather_along(spread(own_panel[:, split:]), torus, 2)
    late = gather_along(late, torus, 1)
    early = gather_along(spread(own_panel[:, :split]), torus, 0)
    trace = torus_sum(trace, torus, (1, 2))
    scaling = width / trace[:1, :1]
    mid0 = gather_along(early[..., :size0], torus, 2)
    mid1 = gather_along(early[..., size0:], torus, 1)
    last = gather_along(late, torus, 0)
    ahead = arrivals(mid0[:1], torus, 1), arrivals(mid1[:1], torus, 2)
    behind = arrivals(mid0[1:], torus, 1), arrivals(mid1[1:], torus, 2)
    plane = blank((1,) + torus[1:] + (rows, panel), jnp.float32)
    panels = blank(torus + (rows, panel), jnp.float32)
    for lane, value, dim in ((0, mid0, 1), (size0, mid1, 2), (split, last, None)):
        at = {} if dim is None else {dim: along(torus, dim)}
        plane = fill(plane, [(value[:1], at)], lane)
        panels = fill(panels, [(value, at)], lane)
    plane = fill(plane, ahead[0], 0)
    plane = fill(plane, ahead[1], size0)
    panels = fill(panels, ahead[0], 0)
    panels = fill(panels, ahead[1], size0)
    panels = fill(panels, moved(behind[0], 1), 0)
    panels = fill(panels, moved(behind[1], 1), size0)
    panels = panels.reshape(width, panel)

    width0, width1, width2 = widths_of(columns)
    fork = width0 + width1
    w_late = gather_along(spread(weights[:, fork:]), torus, 2)
    weights = after(weights, early[:1, :1, :1, :8, :128])
    w_early = gather_along(spread(weights[:, :fork]), torus, 0)
    w_late = gather_along(w_late, torus, 1)
    half0, half1 = width0 // 2, width1 // 2
    w_mids = []
    for turn, (size, dim) in enumerate(((half0, 2), (half1, 1), (width0 - half0, 2), (width1 - half1, 1))):
        first = (0, width0, half0, width0 + half1)[turn]
        w_mids.append(gather_along(w_early[..., first : first + size], torus, dim))
    ends = (1, 2, 1, 2)
    sizes = (half0, half1, width0 - half0, width1 - half1)
    early_columns = width2 + sizes[0] + sizes[1]
    halves = (
        blank(torus + (rows, early_columns), weights.dtype),
        blank(torus + (rows, sizes[2] + sizes[3]), weights.dtype),
    )
    lanes = (width2, width2 + sizes[0], 0, sizes[2])
    pieces = [[(mid, {dim: along(torus, dim)})] for mid, dim in zip(w_mids, ends)]
    first = fill(halves[0], [(w_late, {0: along(torus, 0)})])
    first = fill(fill(first, pieces[0], lanes[0]), pieces[1], lanes[1])
    first = fill(first, arrivals(w_late, torus, 0))
    second = fill(fill(halves[1], pieces[2], lanes[2]), pieces[3], lanes[3])
    received = [arrivals(mid, torus, dim) for mid, dim in zip(w_mids, ends)]
    first = fill(fill(first, received[0], lanes[0]), received[1], lanes[1])
    second = fill(fill(second, received[2], lanes[2]), received[3], lanes[3])
    gathered_weights = [w.reshape(width, -1) for w in (first, second)]

    corner = scaling * plane.reshape(-1, panel)[:panel]
    corner = corner + swapped(corner)
    own = scaling * after(own_panel, early[:1, :1, :1, :8, :128])
    own = own + swapped(own)
    inverse = inverse_factor(corner)
    factored = position < PANEL_STEPS
    lead = lax.dynamic_slice_in_dim(inverse, jnp.minimum(position, PANEL_STEPS - 1) * rows, rows, 0)
    folded = dot(dot(own, inverse, ((1,), (1,)), EXACT), inverse, ((1,), (0,)), EXACT)
    transform = scaling * jnp.where(factored, lead, -folded)
    kept = jnp.where(factored, 0.0, scaling)
    reduced = kept * damped(gram) + dot(transform, panels, ((1,), (1,)), THREE)
    partner = swapped(reduced)
    reduced_gram = reduced + partner

    high = lax.reduce_precision(reduced, 8, 7)
    rest = (reduced - high).astype(jnp.bfloat16)
    both = jnp.concatenate([high.astype(jnp.bfloat16), rest], axis=0)
    solved = []
    for weight in gathered_weights:
        part = jnp.dot(both, weight, preferred_element_type=jnp.float32)
        part = part[:rows] + part[rows:]
        solved.append(part + swapped(part))
    columns_of = [
        solved[0][:, lanes[0] : lanes[1]],
        solved[1][:, : lanes[3]],
        solved[0][:, lanes[1] :],
        solved[1][:, lanes[3] :],
        solved[0][:, :width2],
    ]
    return (reduced_gram, jnp.concatenate(columns_of, axis=1))


def solution(mesh):
    placed = (P("task", "row", None), P("task", "row", None))
    return jax.shard_map(
        per_device,
        mesh=mesh,
        in_specs=placed,
        out_specs=(P("row", None), P("row", None)),
        check_vma=False,
    )
```
